16 devices in a mesh: rep: 4 (over y, z, core), dp: 4 (over x).
Axes of the slice: x: 4, y: 2, z: 1, core: 2. Of those that a mesh axis runs over, the one named last changes fastest.
The devices are a block of a 4x4x8 slice.
Arguments:
- x: bfloat16 [16, 4096, 896], P(('rep', 'dp')), parts along dimension 0
- dy: bfloat16 [16, 4096, 896], P(('rep', 'dp')), parts along dimension 0
- w_gate: bfloat16 [2, 896, 3584], P(None, 'dp')
- w_up: bfloat16 [2, 896, 3584], P(None, 'dp')
- w_down: bfloat16 [2, 3584, 896], P(None, 'dp')
Outputs:
- output 1: bfloat16 [16, 4096, 896], P(('rep', 'dp')), parts along dimension 0
- output 2: bfloat16 [8, 896, 3584], P('rep', 'dp'), parts along dimension 0
- output 3: bfloat16 [8, 896, 3584], P('rep', 'dp'), parts along dimension 0
- output 4: bfloat16 [8, 3584, 896], P('rep', 'dp'), parts along dimension 0
There are 4 independent parts. The reference program is written for one: setup_inputs(seed, part) draws one part's arguments, and reference() takes and returns one part's arrays. A program takes and returns all parts, laid end to end along the dimension named above; an argument that names none is the same for every part.
All inputs are finite; a program needn't handle non-finite values.
Results may differ from the reference program's by a relative error of at most 0.018.
Values are sent between devices in bfloat16 or wider.
A program may use at most 768 MiB of HBM per device.

```python
import jax
import jax.numpy as jnp
from jax import lax

SEQUENCES = 4
TOKENS = 4096
D = 896
FF = 3584
LAYERS = 2
NAMES = ("w_gate", "w_up", "w_down")
SHAPES = {"w_gate": (LAYERS, D, FF), "w_up": (LAYERS, D, FF), "w_down": (LAYERS, FF, D)}


def bump(key, n, height):
    away = (jnp.arange(n, dtype=jnp.int32) - jax.random.randint(key, (), 0, n, jnp.int32)) % n
    return jnp.where(away < n // 8, height, 1.0)


def together(key, own, strength):
    shared = jax.random.normal(key, own.shape[1:], jnp.float32)
    return (own + strength * shared) * lax.rsqrt(1 + strength * strength)


def setup_inputs(seed: int = 0, part: int = 0) -> dict:
    kx, kdy, ka, kb, kz, kf, kh, kl, *kw = jax.random.split(jax.random.key(seed), 8 + len(NAMES))
    kx, kdy, ka, kb = (jax.random.fold_in(k, part) for k in (kx, kdy, ka, kb))
    shape = (SEQUENCES, TOKENS, D)
    much_x, much_dy = jax.random.uniform(kz, (2,), jnp.float32, 0.0, 1.0)
    layers = 2.0 ** jax.random.uniform(kl, (LAYERS, 1, 1), jnp.float32, -1.0, 1.0)
    x = together(ka, jax.random.normal(kx, shape, jnp.float32), much_x) * bump(kf, D, 4.0)
    dy = together(kb, jax.random.normal(kdy, shape, jnp.float32), much_dy)
    drawn = {"x": x.astype(jnp.bfloat16), "dy": (dy * (SEQUENCES * TOKENS) ** -0.5).astype(jnp.bfloat16)}
    for key, name in zip(kw, NAMES, strict=True):
        w = jax.random.normal(key, SHAPES[name], jnp.float32) * SHAPES[name][1] ** -0.5
        drawn[name] = (w * {"w_gate": 1.0, "w_up": bump(kh, FF, 4.0), "w_down": layers}[name]).astype(jnp.bfloat16)
    return drawn


def matmul(a, w):
    return jnp.dot(a, w, preferred_element_type=jnp.float32).astype(jnp.bfloat16)


def normed(h):
    wide = h.astype(jnp.float32)
    scale = lax.rsqrt(jnp.mean(wide**2, -1, keepdims=True) + 1e-6)
    return (wide * scale).astype(jnp.bfloat16)


def layer(h, w):
    a = normed(h)
    gate = jnp.dot(a, w["w_gate"], preferred_element_type=jnp.float32)
    up = jnp.dot(a, w["w_up"], preferred_element_type=jnp.float32)
    return h + matmul((jax.nn.silu(gate) * up).astype(jnp.bfloat16), w["w_down"])


def stack(weights, h):
    return lax.scan(lambda h, w: (layer(h, w), None), h, weights)[0]


def reference(x, dy, w_gate, w_up, w_down):
    weights = dict(zip(NAMES, (w_gate, w_up, w_down), strict=True))

    def take(so_far, sequence):
        h, by_y = sequence
        _, back = jax.vjp(stack, weights, h)
        by_weights, by_h = back(by_y)
        return jax.tree.map(lambda total, term: total + term.astype(jnp.float32), so_far, by_weights), by_h

    none_yet = {name: jnp.zeros(w.shape, jnp.float32) for name, w in weights.items()}
    by_weights, by_x = lax.scan(take, none_yet, (x, dy))
    return (by_x, *(by_weights[name].astype(jnp.bfloat16) for name in NAMES))
```

```python
import functools

import jax
import jax.numpy as jnp
from jax import lax
from jax.experimental import pallas as pl
from jax.experimental.pallas import tpu as pltpu
from jax.sharding import PartitionSpec as P

MESH = pl.DeviceIdType.MESH
BF, F32 = jnp.bfloat16, jnp.float32
LANES = 128
TILE = 1024
SMALL = 512
CHUNK = 256
EPS = 1e-6


def nn(a, b):
    return jnp.dot(a, b, preferred_element_type=F32)


def nt(a, b):
    return lax.dot_general(a, b, (((1,), (1,)), ((), ())), preferred_element_type=F32)


def sigmoid(g):
    return 1.0 / (1.0 + jnp.exp(-g))


def gated_back(g, u, d):
    s = sigmoid(g)
    silu = g * s
    d = d.astype(BF).astype(F32)
    return (silu * u).astype(BF), ((d * u) * (s + silu * (1.0 - s))).astype(BF), (d * silu).astype(BF)


def kernel(
    n, x, dy, wg, wu, wd,
    dx, og, ou, od, a1, a1t, dyt, h1, a2, a2t, dh1, dh1t, g1, u1, gw, gd,
    total, acc_w, acc_d, wgu, wdb, wdt, rows_a, rows_d, cols_a, cols_d, g_buf, u_buf, act, dgu,
    s1_w, s1_d, r1_w, r1_d, s2_w, s2_d, r2_w, r2_d, out_w, out_d,
    ag_send, ag_recv, load_sem, stream_sem, gu_sem, phase_sem, rs_send, rs_recv, out_sem,
):
    tokens, width = x.shape
    layers, depth, ff = wg.shape
    span = n * LANES
    share = ff // n
    blocks = ff // span
    tiles, smalls = tokens // TILE, tokens // SMALL
    half, dhalf = depth // 2, LANES // 2
    gathers = layers * blocks
    me = lax.axis_index("dp")
    rep = lax.axis_index("rep")
    core = rep % 2
    mate = rep + 1 - 2 * core
    right, left, across = (me + 1) % n, (me + n - 1) % n, (me + 2) % n
    to_right, to_left, to_mate = {"dp": right}, {"dp": left}, {"rep": mate}

    def aligned(v, m):
        return pl.multiple_of(v, m)

    def w_rows(owner, c):
        return pl.ds(aligned(owner * depth + c * half, 16), half)

    def d_rows(owner, c):
        return pl.ds(aligned(owner * LANES + c * dhalf, 16), dhalf)

    def remote(src, dst, send, recv, to):
        return pltpu.make_async_remote_copy(src_ref=src, dst_ref=dst, send_sem=send, recv_sem=recv, device_id=to, device_id_type=MESH)

    def wait_like(ref, sem):
        pltpu.make_async_copy(ref, ref, sem).wait()

    def sends_done(k, m):
        i = m % 4
        if k < 2:
            wait_like(gw.at[m, :, w_rows(me, core), :], ag_send.at[k, 0, i])
            wait_like(gd.at[m, d_rows(me, core), :], ag_send.at[k, 1, i])
        elif k < 4:
            wait_like(gw.at[m, :, w_rows(me, core), pl.ds(0, span // 2)], ag_send.at[k, 0, i])
            wait_like(gd.at[m, pl.ds(0, dhalf // 2), :], ag_send.at[k, 1, i])
        else:
            wait_like(gw.at[m, :, pl.ds(0, 3 * half), :], ag_send.at[k, 0, i])
            wait_like(gd.at[m, pl.ds(0, 3 * dhalf), :], ag_send.at[k, 1, i])

    def give(m):
        layer, b = m // blocks, m % blocks

        @pl.when(m >= 4)
        def _():
            sends_done(0, m - 4)
            sends_done(1, m - 4)

        i = m % 4
        for k, to in ((0, to_right), (1, to_left)):
            for j, w in enumerate((wg, wu)):
                for group in range(n):
                    at = pl.ds(aligned(group * share + b * LANES, LANES), LANES)
                    remote(
                        w.at[layer, pl.ds(aligned(core * half, 16), half), at],
                        gw.at[m, j, w_rows(me, core), pl.ds(group * LANES, LANES)],
                        ag_send.at[k, 0, i], ag_recv.at[k, 0, m], to,
                    ).start()
            remote(
                wd.at[layer, pl.ds(aligned(b * LANES + core * dhalf, 16), dhalf), :],
                gd.at[m, d_rows(me, core), :],
                ag_send.at[k, 1, i], ag_recv.at[k, 1, m], to,
            ).start()

    def swap(m, owner):
        w, d = gw.at[m, :, w_rows(owner, core), :], gd.at[m, d_rows(owner, core), :]
        remote(w, w, ag_send.at[4, 0, m % 4], ag_recv.at[4, 0, m], to_mate).start()
        remote(d, d, ag_send.at[4, 1, m % 4], ag_recv.at[4, 1, m], to_mate).start()

    def pass_on(m):
        i = m % 4

        @pl.when(m >= 4)
        def _():
            for k in (2, 3, 4):
                sends_done(k, m - 4)

        for k, owner in ((0, left), (1, right)):
            wait_like(gw.at[m, :, w_rows(owner, core), :], ag_recv.at[k, 0, m])
            wait_like(gd.at[m, d_rows(owner, core), :], ag_recv.at[k, 1, m])
        for k, owner, to, part in ((2, left, to_right, 0), (3, right, to_left, 1)):
            w = gw.at[m, :, w_rows(owner, core), pl.ds(part * (span // 2), span // 2)]
            d = gd.at[m, pl.ds(aligned(owner * LANES + core * dhalf + part * (dhalf // 2), 16), dhalf // 2), :]
            remote(w, w, ag_send.at[k, 0, i], ag_recv.at[k, 0, m], to).start()
            remote(d, d, ag_send.at[k, 1, i], ag_recv.at[k, 1, m], to).start()
        swap(m, left)
        swap(m, right)

    def pass_across(m):
        for k, part in ((2, 0), (3, 1)):
            wait_like(gw.at[m, :, w_rows(across, core), pl.ds(part * (span // 2), span // 2)], ag_recv.at[k, 0, m])
            wait_like(gd.at[m, pl.ds(aligned(across * LANES + core * dhalf + part * (dhalf // 2), 16), dhalf // 2), :], ag_recv.at[k, 1, m])
        swap(m, across)

    def gathered(m):
        wait_like(gw.at[m, :, pl.ds(0, 3 * half), :], ag_recv.at[4, 0, m])
        wait_like(gd.at[m, pl.ds(0, 3 * dhalf), :], ag_recv.at[4, 1, m])

    def load(m, slot):
        layer, b = m // blocks, m % blocks
        for owner in (left, right, across):
            r, d = pl.ds(aligned(owner * depth, 32), depth), pl.ds(aligned(owner * LANES, LANES), LANES)
            pltpu.make_async_copy(gw.at[m, :, r, :], wgu.at[slot, :, r, :], load_sem.at[0]).start()
            pltpu.make_async_copy(gd.at[m, d, :], wdb.at[d, :], load_sem.at[1]).start()
        r = pl.ds(aligned(me * depth, 32), depth)
        for j, w in enumerate((wg, wu)):
            for group in range(n):
                at = pl.ds(aligned(group * share + b * LANES, LANES), LANES)
                pltpu.make_async_copy(
                    w.at[layer, :, at], wgu.at[slot, j, r, pl.ds(group * LANES, LANES)], load_sem.at[0]
                ).start()
        pltpu.make_async_copy(
            wd.at[layer, pl.ds(aligned(b * LANES, LANES), LANES), :],
            wdb.at[pl.ds(aligned(me * LANES, LANES), LANES), :], load_sem.at[1],
        ).start()

    def loaded(slot):
        wait_like(wgu.at[slot], load_sem.at[0])
        wait_like(wdb, load_sem.at[1])
        for c in range(span // LANES):
            at = pl.ds(c * LANES, LANES)
            wdt[:, at] = wdb[at, :].T

    def gather_ticks(m, t):
        more = m + 1 < gathers

        @pl.when((t == 0) & more)
        def _():
            pass_on(m + 1)

        @pl.when((t == 0) & (m < blocks))
        def _():
            give(m + 3)

        @pl.when((t == 0) & (m == blocks))
        def _():
            lax.fori_loop(blocks + 3, gathers, lambda k, _: give(k), None)

        @pl.when((t == 2) & more)
        def _():
            pass_across(m + 1)

        @pl.when(t == 3)
        def _():
            @pl.when(more)
            def _():
                gathered(m + 1)

            load((m + 1) % gathers, (m + 1) % 2)

    def own_w(p, j, owner, part=None):
        at = slice(None) if part is None else pl.ds(part * (span // 2), span // 2)
        return acc_w[p, j, pl.ds(aligned(owner * depth, 32), depth), at]

    def own_d(p, owner, part=None):
        at = slice(None) if part is None else pl.ds(part * (width // 2), width // 2)
        return acc_d[p, at, pl.ds(aligned(owner * LANES, LANES), LANES)]

    def w_half(ref, part):
        return ref.at[:, :, pl.ds(part * (span // 2), span // 2)]

    def d_half(ref, part):
        return ref.at[pl.ds(part * (width // 2), width // 2), :]

    def first_copies():
        for part, to in ((0, to_right), (1, to_left)):
            yield remote(w_half(s1_w, part), w_half(r1_w, part), rs_send.at[0, part, 0], rs_recv.at[0, part, 0], to)
            yield remote(d_half(s1_d, part), d_half(r1_d, part), rs_send.at[0, part, 1], rs_recv.at[0, part, 1], to)

    def second_copies():
        for part, to in ((0, to_right), (1, to_left)):
            yield remote(s2_w.at[part], r2_w.at[part], rs_send.at[1, part, 0], rs_recv.at[1, part, 0], to)
            yield remote(s2_d.at[part], r2_d.at[part], rs_send.at[1, part, 1], rs_recv.at[1, part, 1], to)

    def reduce_start(r):
        p = r % 2
        for j in range(2):
            s1_w[j] = own_w(p, j, across).astype(BF)
        s1_d[...] = own_d(p, across).astype(BF)
        for copy in first_copies():
            copy.start()

    def reduce_middle(r):
        p = r % 2
        for copy in first_copies():
            copy.wait()
        for part, owner in ((0, right), (1, left)):
            for j in range(2):
                came, plain = pl.ds(part * (span // 2), span // 2), pl.ds((1 - part) * (span // 2), span // 2)
                s2_w[part, j, :, came] = (own_w(p, j, owner, part) + r1_w[j, :, came].astype(F32)).astype(BF)
                s2_w[part, j, :, plain] = own_w(p, j, owner, 1 - part).astype(BF)
            came, plain = pl.ds(part * (width // 2), width // 2), pl.ds((1 - part) * (width // 2), width // 2)
            s2_d[part, came, :] = (own_d(p, owner, part) + r1_d[came, :].astype(F32)).astype(BF)
            s2_d[part, plain, :] = own_d(p, owner, 1 - part).astype(BF)
        for copy in second_copies():
            copy.start()

    def result_copies(r):
        layer, b = layers - 1 - r // blocks, r % blocks
        for j, o in enumerate((og, ou)):
            for group in range(n):
                at = pl.ds(aligned(group * share + b * LANES, LANES), LANES)
                yield pltpu.make_async_copy(out_w.at[j, :, pl.ds(group * LANES, LANES)], o.at[layer, :, at], out_sem.at[j, group])
        yield pltpu.make_async_copy(out_d, od.at[layer, pl.ds(aligned(b * LANES, LANES), LANES), :], out_sem.at[2, 0])

    def reduce_end(r):
        p = r % 2
        for copy in second_copies():
            copy.wait()

        @pl.when(r >= 1)
        def _():
            for copy in result_copies(r - 1):
                copy.wait()

        for j in range(2):
            out_w[j] = (own_w(p, j, me) + r2_w[0, j].astype(F32) + r2_w[1, j].astype(F32)).astype(BF)
        mine = (own_d(p, me) + r2_d[0].astype(F32) + r2_d[1].astype(F32)).astype(BF)
        out_d[...] = mine.T
        for copy in result_copies(r):
            copy.start()

    def token_rows(ref, t, size):
        return ref.at[pl.ds(aligned(t * size, size), size), :]

    def token_cols(ref, t, size):
        return ref.at[:, pl.ds(aligned(t * size, size), size)]

    def copies(pairs, slot):
        for k, (src, dst) in enumerate(pairs):
            yield pltpu.make_async_copy(src, dst, stream_sem.at[k, slot])

    def start(pairs, slot):
        for copy in copies(pairs, slot):
            copy.start()

    def wait(pairs, slot):
        for copy in copies(pairs, slot):
            copy.wait()

    def norm_scale(wide):
        return lax.rsqrt(jnp.sum(wide * wide, -1, keepdims=True) * (1.0 / width) + EPS)

    def norm_back(h, da):
        wide = h.astype(F32)
        scale = norm_scale(wide)
        inner = jnp.sum(da * wide, -1, keepdims=True)
        return da * scale - wide * (scale * scale * scale * inner * (1.0 / width))

    def passes(ins, outs, chunk, between=()):
        def put(t, slot):
            for k, (src, dst) in enumerate(outs(t, slot)):
                yield pltpu.make_async_copy(src, dst, phase_sem.at[k, slot])

        start(ins(0, 0), 0)
        for t in range(tiles):
            slot = t % 2
            if t >= 1:
                for copy in put(t - 1, 1 - slot):
                    copy.wait()
            if t + 1 < tiles:
                start(ins(t + 1, 1 - slot), 1 - slot)
            wait(ins(t, slot), slot)

            def one(c, _):
                at = pl.ds(aligned(c * LANES, LANES), LANES)
                chunk(slot, at, pl.ds(aligned(t * TILE + c * LANES, LANES), LANES))

            lax.fori_loop(0, TILE // LANES, one, None)
            for copy in put(t, slot):
                copy.start()
            for after, act_ in between:
                if after == t:
                    act_()
        for copy in put(tiles - 1, (tiles - 1) % 2):
            copy.wait()

    barrier = pltpu.get_barrier_semaphore()
    for to in (to_right, to_left, to_mate):
        pl.semaphore_signal(barrier, inc=1, device_id=to, device_id_type=MESH)
    pl.semaphore_wait(barrier, 3)
    give(0)

    def enter(slot, at, _):
        wide = rows_a[slot, at, :].astype(F32)
        a = (wide * norm_scale(wide)).astype(BF)
        rows_a[slot, at, :] = a
        cols_a[slot, :, at] = a.T
        cols_d[slot, :, at] = rows_d[slot, at, :].T

    def first_pass():
        pass_on(0)
        give(1)
        give(2)

    def first_load():
        gathered(0)
        load(0, 0)

    passes(
        lambda t, s: [(token_rows(x, t, TILE), rows_a.at[s]), (token_rows(dy, t, TILE), rows_d.at[s])],
        lambda t, s: [
            (rows_a.at[s], token_rows(a1, t, TILE)), (cols_a.at[s], token_cols(a1t, t, TILE)), (cols_d.at[s], token_cols(dyt, t, TILE)),
        ],
        enter,
        [(1, first_pass), (2, lambda: pass_across(0)), (3, first_load)],
    )

    def add_total(at, first, value):
        total[:, at] = value + jnp.where(first, 0.0, total[:, at])

    def f1_in(s, slot):
        return [(token_rows(a1, s % tiles, TILE), rows_a.at[slot])]

    def gu_copies(m, t, h):
        at = pl.ds(aligned(t * TILE + h * SMALL, SMALL), SMALL)
        yield pltpu.make_async_copy(g_buf.at[h], g1.at[m, at, :], gu_sem.at[0, h])
        yield pltpu.make_async_copy(u_buf.at[h], u1.at[m, at, :], gu_sem.at[1, h])

    def f1_step(s, _):
        m, t, slot = s // tiles, s % tiles, s % 2
        gather_ticks(m, t)

        @pl.when(t == 0)
        def _():
            loaded(m % 2)

        @pl.when(s + 1 < blocks * tiles)
        def _():
            start(f1_in(s + 1, 1 - slot), 1 - slot)

        wait(f1_in(s, slot), slot)
        w = wgu.at[m % 2]
        for h in range(TILE // SMALL):
            @pl.when(s > 0)
            def _():
                for copy in gu_copies(m, t, h):
                    copy.wait()

            for c in range(SMALL // CHUNK):
                r, own = pl.ds(h * SMALL + c * CHUNK, CHUNK), pl.ds(c * CHUNK, CHUNK)
                a = rows_a[slot, r, :]
                g, u = nn(a, w[0]), nn(a, w[1])
                g_buf[h, own, :] = g
                u_buf[h, own, :] = u
                act[r, :] = (g * sigmoid(g) * u).astype(BF)
            for copy in gu_copies(m, t, h):
                copy.start()
        add_total(pl.ds(aligned(t * TILE, TILE), TILE), m == 0, nt(wdt[...], act[...]))

    start(f1_in(0, 0), 0)
    lax.fori_loop(0, blocks * tiles, f1_step, None)
    for h in range(TILE // SMALL):
        for copy in gu_copies(blocks - 1, tiles - 1, h):
            copy.wait()

    def turn(slot, at, tok):
        h = rows_d[slot, at, :].astype(F32) + total[:, tok].astype(BF).T.astype(F32)
        h = h.astype(BF)
        rows_d[slot, at, :] = h
        wide = h.astype(F32)
        a = (wide * norm_scale(wide)).astype(BF)
        rows_a[slot, at, :] = a
        cols_a[slot, :, at] = a.T

    passes(
        lambda t, s: [(token_rows(x, t, TILE), rows_d.at[s])],
        lambda t, s: [
            (rows_d.at[s], token_rows(h1, t, TILE)), (rows_a.at[s], token_rows(a2, t, TILE)), (cols_a.at[s], token_cols(a2t, t, TILE)),
        ],
        turn,
    )

    def fold(p, tok, size, first_step, first_block, slot, w):
        r = pl.ds(0, size)
        add_total(tok, first_block, nt(w[0], dgu[0, r, :]) + nt(w[1], dgu[1, r, :]))
        for j in range(2):
            acc_w[p, j] = nn(cols_a[slot, :, r], dgu[j, r, :]) + jnp.where(first_step, 0.0, acc_w[p, j])
        acc_d[p] = nn(cols_d[slot, :, r], act[r, :]) + jnp.where(first_step, 0.0, acc_d[p])

    def f2_in(s, slot):
        t = s % tiles
        return [
            (token_rows(a2, t, TILE), rows_a.at[slot]), (token_rows(dy, t, TILE), rows_d.at[slot]),
            (token_cols(a2t, t, TILE), cols_a.at[slot]), (token_cols(dyt, t, TILE), cols_d.at[slot]),
        ]

    def f2_step(s, _):
        r, t, slot = s // tiles, s % tiles, s % 2
        m = blocks + r
        gather_ticks(m, t)

        @pl.when((t == 2) & (r >= 1))
        def _():
            reduce_middle(r - 1)

        @pl.when(t == 0)
        def _():
            loaded(m % 2)

        @pl.when(s + 1 < blocks * tiles)
        def _():
            start(f2_in(s + 1, 1 - slot), 1 - slot)

        wait(f2_in(s, slot), slot)
        w = wgu.at[m % 2]

        def products(c):
            at = pl.ds(c * CHUNK, CHUNK)
            a = rows_a[slot, at, :]
            return nn(a, w[0]), nn(a, w[1]), nn(rows_d[slot, at, :], wdt[...])

        def keep(c, values):
            at = pl.ds(c * CHUNK, CHUNK)
            act[at, :], dgu[0, at, :], dgu[1, at, :] = gated_back(*values)

        before = products(0)
        for c in range(1, TILE // CHUNK):
            now = products(c)
            keep(c - 1, before)
            before = now
        keep(TILE // CHUNK - 1, before)
        fold(r % 2, pl.ds(aligned(t * TILE, TILE), TILE), TILE, t == 0, r == 0, slot, w)

        @pl.when(t == tiles - 1)
        def _():
            @pl.when(r >= 1)
            def _():
                reduce_end(r - 1)

            reduce_start(r)

    start(f2_in(0, 0), 0)
    lax.fori_loop(0, blocks * tiles, f2_step, None)

    def back(slot, at, tok):
        da = total[:, tok].astype(BF).T.astype(F32)
        grad = norm_back(rows_a[slot, at, :], da).astype(BF).astype(F32)
        d = (rows_d[slot, at, :].astype(F32) + grad).astype(BF)
        rows_d[slot, at, :] = d
        return d

    def back_both(slot, at, tok):
        cols_d[slot, :, at] = back(slot, at, tok).T

    passes(
        lambda t, s: [(token_rows(h1, t, TILE), rows_a.at[s]), (token_rows(dy, t, TILE), rows_d.at[s])],
        lambda t, s: [(rows_d.at[s], token_rows(dh1, t, TILE)), (cols_d.at[s], token_cols(dh1t, t, TILE))],
        back_both,
    )

    def b1_in(s, slot):
        b, t = s // smalls, s % smalls
        some = pl.ds(0, SMALL)
        return [
            (token_rows(dh1, t, SMALL), rows_d.at[slot, some, :]),
            (token_cols(a1t, t, SMALL), cols_a.at[slot, :, some]), (token_cols(dh1t, t, SMALL), cols_d.at[slot, :, some]),
            (token_rows(g1.at[b], t, SMALL), g_buf.at[slot]), (token_rows(u1.at[b], t, SMALL), u_buf.at[slot]),
        ]

    def b1_step(s, _):
        b, t, slot = s // smalls, s % smalls, s % 2
        m, r = gathers + b, blocks + b

        @pl.when((t == 1) & (b + 1 < blocks))
        def _():
            load(b + 1, (m + 1) % 2)

        @pl.when(t == smalls // 2)
        def _():
            reduce_middle(r - 1)

        @pl.when(t == 0)
        def _():
            loaded(m % 2)

        @pl.when(s + 1 < blocks * smalls)
        def _():
            start(b1_in(s + 1, 1 - slot), 1 - slot)

        wait(b1_in(s, slot), slot)
        w = wgu.at[m % 2]
        for c in range(SMALL // CHUNK):
            at = pl.ds(c * CHUNK, CHUNK)
            d = nn(rows_d[slot, at, :], wdt[...])
            act[at, :], dgu[0, at, :], dgu[1, at, :] = gated_back(g_buf[slot, at, :], u_buf[slot, at, :], d)
        fold(r % 2, pl.ds(aligned(t * SMALL, SMALL), SMALL), SMALL, t == 0, b == 0, slot, w)

        @pl.when(t == smalls - 1)
        def _():
            reduce_end(r - 1)
            reduce_start(r)

    start(b1_in(0, 0), 0)
    lax.fori_loop(0, blocks * smalls, b1_step, None)

    last = layers * blocks - 1

    def leave(slot, at, tok):
        back(slot, at, tok)

    passes(
        lambda t, s: [(token_rows(x, t, TILE), rows_a.at[s]), (token_rows(dh1, t, TILE), rows_d.at[s])],
        lambda t, s: [(rows_d.at[s], token_rows(dx, t, TILE))],
        leave,
        [(2, lambda: reduce_middle(last))],
    )
    reduce_end(last)
    for copy in result_copies(last):
        copy.wait()
    for m in range(max(gathers - 4, 0), gathers):
        for k in range(5):
            sends_done(k, m)


def solution(mesh):
    n = mesh.shape["dp"]

    def local(x, dy, wg, wu, wd):
        tokens, width = x.shape[1:]
        layers, depth, ff = wg.shape
        span = n * LANES
        blocks = ff // span
        assert n == 4 and layers == 2 and mesh.shape["rep"] % 2 == 0
        assert ff % span == 0 and tokens % TILE == 0 and tokens // TILE == 4
        wide, tall = jax.ShapeDtypeStruct((tokens, width), BF), jax.ShapeDtypeStruct((width, tokens), BF)
        kept = jax.ShapeDtypeStruct((blocks, tokens, span), F32)
        grads = [jax.ShapeDtypeStruct(w.shape, w.dtype) for w in (wg, wu, wd)]
        hbm = [
            wide, tall, tall, wide, wide, tall, wide, tall, kept, kept,
            jax.ShapeDtypeStruct((layers * blocks, 2, width, span), BF), jax.ShapeDtypeStruct((layers * blocks, span, width), BF),
        ]
        outs = [wide, *grads, *hbm]
        dma = pltpu.SemaphoreType.DMA
        flops = 2 * tokens * width * ff * (9 * layers - 1)
        got = pl.pallas_call(
            functools.partial(kernel, n),
            out_shape=outs,
            in_specs=[pl.BlockSpec(memory_space=pl.ANY)] * 5,
            out_specs=[pl.BlockSpec(memory_space=pl.ANY)] * len(outs),
            scratch_shapes=[
                pltpu.VMEM((width, tokens), F32),
                pltpu.VMEM((2, 2, width, span), F32), pltpu.VMEM((2, width, span), F32),
                pltpu.VMEM((2, 2, width, span), BF), pltpu.VMEM((span, width), BF), pltpu.VMEM((width, span), BF),
                pltpu.VMEM((2, TILE, width), BF), pltpu.VMEM((2, TILE, width), BF),
                pltpu.VMEM((2, width, TILE), BF), pltpu.VMEM((2, width, TILE), BF),
                pltpu.VMEM((2, SMALL, span), F32), pltpu.VMEM((2, SMALL, span), F32),
                pltpu.VMEM((TILE, span), BF), pltpu.VMEM((2, TILE, span), BF),
                pltpu.VMEM((2, depth, span), BF), pltpu.VMEM((width, LANES), BF),
                pltpu.VMEM((2, depth, span), BF), pltpu.VMEM((width, LANES), BF),
                pltpu.VMEM((2, 2, depth, span), BF), pltpu.VMEM((2, width, LANES), BF),
                pltpu.VMEM((2, 2, depth, span), BF), pltpu.VMEM((2, width, LANES), BF),
                pltpu.VMEM((2, depth, span), BF), pltpu.VMEM((LANES, width), BF),
                dma((5, 2, 4)), dma((5, 2, layers * blocks)), dma((2,)), dma((5, 2)), dma((2, 2)), dma((3, 2)),
                dma((2, 2, 2)), dma((2, 2, 2)), dma((3, n)),
            ],
            compiler_params=pltpu.CompilerParams(collective_id=0, has_side_effects=True, vmem_limit_bytes=67043328),
            cost_estimate=pl.CostEstimate(flops=flops, bytes_accessed=0, transcendentals=0),
            name="stack",
        )(x[0], dy[0], wg, wu, wd)
        return (got[0][None], *got[1:4])

    tok, row = P(("rep", "dp"), None, None), P(None, "dp", None)
    return jax.shard_map(
        local, mesh=mesh, in_specs=(tok, tok, row, row, row), out_specs=(tok, *[P("rep", "dp", None)] * 3), check_vma=False
    )
```

```python
import functools

import jax
import jax.numpy as jnp
from jax import lax
from jax.experimental import pallas as pl
from jax.experimental.pallas import tpu as pltpu
from jax.sharding import PartitionSpec as P

MESH = pl.DeviceIdType.MESH
BF, F32 = jnp.bfloat16, jnp.float32
LANES = 128
TILE = 1024
CHUNK = 256
STRIP = 256
SOON, LATER = (0,), (1, 2)
ALL = (0, 1, 2)
EPS = 1e-6


def nn(a, b):
    return jnp.dot(a, b, preferred_element_type=F32)


def nt(a, b):
    return lax.dot_general(a, b, (((1,), (1,)), ((), ())), preferred_element_type=F32)


def sigmoid(g):
    return 1.0 / (1.0 + jnp.exp(-g))


def gated_back(g, u, d):
    s = sigmoid(g)
    silu = g * s
    d = d.astype(BF).astype(F32)
    return (silu * u).astype(BF), ((d * u) * (s + silu * (1.0 - s))).astype(BF), (d * silu).astype(BF)


def kernel(
    n, x, dy, wg, wu, wd,
    dx, og, ou, od, a1, a1t, dyt, h1t, a2, a2t, dh1, dh1t, g1, u1, gw, gd,
    total, acc_w, acc_d, wgu, wdb, wdt, rows_a, rows_d, cols_a, cols_d, g_buf, u_buf, act, dgu,
    r1_w, r1_d, s2_w, s2_d, r2_w, r2_d, out_w, out_d,
    ag_send, ag_recv, load_sem, stream_sem, gu_sem, phase_sem, tall_sem, h1_sem, rs_send, rs_recv, out_sem,
):
    tokens, width = x.shape
    layers, depth, ff = wg.shape
    span = n * LANES
    share = ff // n
    blocks = ff // span
    tiles = tokens // TILE
    part_tile = TILE // 2
    half, dhalf = depth // 2, LANES // 2
    gathers = layers * blocks
    me = lax.axis_index("dp")
    rep = lax.axis_index("rep")
    core = rep % 2
    mate = rep + 1 - 2 * core
    right, left, across = (me + 1) % n, (me + n - 1) % n, (me + 2) % n
    to_right, to_left, to_mate = {"dp": right}, {"dp": left}, {"rep": mate}

    def aligned(v, m):
        return pl.multiple_of(v, m)

    def w_rows(owner, c):
        return pl.ds(aligned(owner * depth + c * half, 16), half)

    def d_rows(owner, c):
        return pl.ds(aligned(owner * LANES + c * dhalf, 16), dhalf)

    def remote(src, dst, send, recv, to):
        return pltpu.make_async_remote_copy(src_ref=src, dst_ref=dst, send_sem=send, recv_sem=recv, device_id=to, device_id_type=MESH)

    def wait_like(ref, sem):
        pltpu.make_async_copy(ref, ref, sem).wait()

    def piece(m, item, owner, part=None):
        if item < 2:
            return gw.at[m, item, w_rows(owner, core), pl.ds(0, span) if part is None else pl.ds(part * (span // 2), span // 2)]
        if part is None:
            return gd.at[m, d_rows(owner, core), :]
        return gd.at[m, pl.ds(aligned(owner * LANES + core * dhalf + part * (dhalf // 2), 16), dhalf // 2), :]

    def three_pieces(m, item):
        return gw.at[m, item, pl.ds(0, 3 * half), :] if item < 2 else gd.at[m, pl.ds(0, 3 * dhalf), :]

    def sends_done(k, m, items):
        for item in items:
            ref = three_pieces(m, item) if k == 4 else piece(m, item, me, None if k < 2 else 0)
            wait_like(ref, ag_send.at[k, item, m % 4])

    def give(m, items):
        layer, b = m // blocks, m % blocks

        @pl.when(m >= 4)
        def _():
            sends_done(0, m - 4, items)
            sends_done(1, m - 4, items)

        for item in items:
            for k, to in ((0, to_right), (1, to_left)):
                send, recv = ag_send.at[k, item, m % 4], ag_recv.at[k, item, m]
                if item == 2:
                    rows = pl.ds(aligned(b * LANES + core * dhalf, 16), dhalf)
                    remote(wd.at[layer, rows, :], piece(m, item, me), send, recv, to).start()
                    continue
                for group in range(n):
                    at = pl.ds(aligned(group * share + b * LANES, LANES), LANES)
                    remote(
                        (wg, wu)[item].at[layer, pl.ds(aligned(core * half, 16), half), at],
                        gw.at[m, item, w_rows(me, core), pl.ds(group * LANES, LANES)], send, recv, to,
                    ).start()

    def swap(m, owner, items):
        for item in items:
            ref = piece(m, item, owner)
            remote(ref, ref, ag_send.at[4, item, m % 4], ag_recv.at[4, item, m], to_mate).start()

    def pass_on(m, items):
        @pl.when(m >= 4)
        def _():
            for k in (2, 3, 4):
                sends_done(k, m - 4, items)

        for item in items:
            for k, owner, to in ((0, left, to_right), (1, right, to_left)):
                wait_like(piece(m, item, owner), ag_recv.at[k, item, m])
                ref = piece(m, item, owner, k)
                remote(ref, ref, ag_send.at[k + 2, item, m % 4], ag_recv.at[k + 2, item, m], to).start()
        swap(m, left, items)
        swap(m, right, items)

    def pass_across(m, items):
        for item in items:
            for part in range(2):
                wait_like(piece(m, item, across, part), ag_recv.at[part + 2, item, m])
        swap(m, across, items)

    def gathered(m):
        for item in ALL:
            wait_like(three_pieces(m, item), ag_recv.at[4, item, m])

    def load(m, slot):
        layer, b = m // blocks, m % blocks
        for owner in (left, right, across):
            r, d = pl.ds(aligned(owner * depth, 32), depth), pl.ds(aligned(owner * LANES, LANES), LANES)
            pltpu.make_async_copy(gw.at[m, :, r, :], wgu.at[slot, :, r, :], load_sem.at[0]).start()
            pltpu.make_async_copy(gd.at[m, d, :], wdb.at[d, :], load_sem.at[1]).start()
        r = pl.ds(aligned(me * depth, 32), depth)
        for j, w in enumerate((wg, wu)):
            for group in range(n):
                at = pl.ds(aligned(group * share + b * LANES, LANES), LANES)
                pltpu.make_async_copy(
                    w.at[layer, :, at], wgu.at[slot, j, r, pl.ds(group * LANES, LANES)], load_sem.at[0]
                ).start()
        pltpu.make_async_copy(
            wd.at[layer, pl.ds(aligned(b * LANES, LANES), LANES), :],
            wdb.at[pl.ds(aligned(me * LANES, LANES), LANES), :], load_sem.at[1],
        ).start()

    def loaded(slot):
        wait_like(wgu.at[slot], load_sem.at[0])
        wait_like(wdb, load_sem.at[1])
        for c in range(span // LANES):
            at = pl.ds(c * LANES, LANES)
            wdt[:, at] = wdb[at, :].T

    def gather_ticks(m, t):
        more = m + 1 < gathers
        first = m == 0

        @pl.when((t == 0) & more)
        def _():
            pass_on(m + 1, SOON)

        @pl.when((t == jnp.where(first, 1, 0)) & more)
        def _():
            pass_on(m + 1, LATER)

            @pl.when(m + 2 < gathers)
            def _():
                give(m + 2, ALL)

        @pl.when((t == jnp.where(first, 3, 2)) & more)
        def _():
            pass_across(m + 1, ALL)

        @pl.when(t == 3)
        def _():
            @pl.when(more)
            def _():
                gathered(m + 1)

            load((m + 1) % gathers, (m + 1) % 2)

    def own_w(p, j, owner, part=None):
        at = slice(None) if part is None else pl.ds(part * (span // 2), span // 2)
        return acc_w[p, j, pl.ds(aligned(owner * depth, 32), depth), at]

    def own_d(p, owner, part=None):
        at = slice(None) if part is None else pl.ds(part * (width // 2), width // 2)
        return acc_d[p, at, pl.ds(aligned(owner * LANES, LANES), LANES)]

    def item_half(ref_w, ref_d, item, part):
        if item < 2:
            return ref_w.at[item, :, pl.ds(part * (span // 2), span // 2)]
        return ref_d.at[pl.ds(part * (width // 2), width // 2), :]

    def first_copies(items):
        for item in items:
            for part, to in ((0, to_right), (1, to_left)):
                yield remote(
                    item_half(s2_w.at[1], s2_d.at[1], item, part), item_half(r1_w, r1_d, item, part),
                    rs_send.at[0, part, item], rs_recv.at[0, part, item], to,
                )

    def second_copies(items):
        for item in items:
            for part, to in ((0, to_right), (1, to_left)):
                src, dst = (s2_w.at[part, item], r2_w.at[part, item]) if item < 2 else (s2_d.at[part], r2_d.at[part])
                yield remote(src, dst, rs_send.at[1, part, item], rs_recv.at[1, part, item], to)

    def reduce_start(r):
        p = r % 2
        for j in range(2):
            s2_w[1, j] = own_w(p, j, across).astype(BF)
        s2_d[1] = own_d(p, across).astype(BF)
        for copy in first_copies(ALL):
            copy.start()

    def reduce_middle(r, items):
        p = r % 2
        for copy in first_copies(items):
            copy.wait()
        for part, owner in ((0, right), (1, left)):
            for j in items:
                size = (span if j < 2 else width) // 2
                came, plain = pl.ds(part * size, size), pl.ds((1 - part) * size, size)
                if j < 2:
                    s2_w[part, j, :, came] = (own_w(p, j, owner, part) + r1_w[j, :, came].astype(F32)).astype(BF)
                    s2_w[part, j, :, plain] = own_w(p, j, owner, 1 - part).astype(BF)
                else:
                    s2_d[part, came, :] = (own_d(p, owner, part) + r1_d[came, :].astype(F32)).astype(BF)
                    s2_d[part, plain, :] = own_d(p, owner, 1 - part).astype(BF)
        for copy in second_copies(items):
            copy.start()

    def result_copies(r):
        layer, b = layers - 1 - r // blocks, r % blocks
        for j, o in enumerate((og, ou)):
            for group in range(n):
                at = pl.ds(aligned(group * share + b * LANES, LANES), LANES)
                yield pltpu.make_async_copy(out_w.at[j, :, pl.ds(group * LANES, LANES)], o.at[layer, :, at], out_sem.at[j, group])
        yield pltpu.make_async_copy(out_d, od.at[layer, pl.ds(aligned(b * LANES, LANES), LANES), :], out_sem.at[2, 0])

    def reduce_end(r):
        p = r % 2
        for copy in second_copies(ALL):
            copy.wait()

        @pl.when(r >= 1)
        def _():
            for copy in result_copies(r - 1):
                copy.wait()

        for j in range(2):
            out_w[j] = (own_w(p, j, me) + r2_w[0, j].astype(F32) + r2_w[1, j].astype(F32)).astype(BF)
        mine = (own_d(p, me) + r2_d[0].astype(F32) + r2_d[1].astype(F32)).astype(BF)
        out_d[...] = mine.T
        for copy in result_copies(r):
            copy.start()

    def token_rows(ref, t):
        return ref.at[pl.ds(aligned(t * TILE, TILE), TILE), :]

    def token_cols(ref, t):
        return ref.at[:, pl.ds(aligned(t * TILE, TILE), TILE)]

    def half_cols(ref, t, h):
        return ref.at[:, pl.ds(aligned(t * TILE + h * part_tile, part_tile), part_tile)]

    def copies(pairs, slot, sem=stream_sem):
        for k, (src, dst) in enumerate(pairs):
            yield pltpu.make_async_copy(src, dst, sem.at[k, slot])

    def start(pairs, slot, sem=stream_sem):
        for copy in copies(pairs, slot, sem):
            copy.start()

    def wait(pairs, slot, sem=stream_sem):
        for copy in copies(pairs, slot, sem):
            copy.wait()

    def norm_scale(wide, axis):
        return lax.rsqrt(jnp.sum(wide * wide, axis, keepdims=True) * (1.0 / width) + EPS)

    def norm_back(h, da, axis):
        wide = h.astype(F32)
        scale = norm_scale(wide, axis)
        inner = jnp.sum(da * wide, axis, keepdims=True)
        return da * scale - wide * (scale * scale * scale * inner * (1.0 / width))

    def strips(t, h, body):
        def one(c, _):
            def at(first):
                return pl.ds(aligned(first + c * STRIP, STRIP), STRIP)

            body(at(0), at(h * part_tile), at(t * TILE + h * part_tile))

        lax.fori_loop(0, part_tile // STRIP, one, None)

    def passes(ins, outs, body, between):
        def tile(t, _):
            slot = t % 2
            wait(ins(t, slot), slot)
            strips(t, 0, functools.partial(body, slot))

            @pl.when(t >= 1)
            def _():
                wait(outs(t - 1, 1 - slot), 1 - slot, phase_sem)

            @pl.when(t + 1 < tiles)
            def _():
                start(ins(t + 1, 1 - slot), 1 - slot)

            strips(t, 1, functools.partial(body, slot))
            start(outs(t, slot), slot, phase_sem)
            for after, do in between:
                pl.when(t == after)(do)

        start(ins(0, 0), 0)
        lax.fori_loop(0, tiles, tile, None)

    barrier = pltpu.get_barrier_semaphore()
    for to in (to_right, to_left, to_mate):
        pl.semaphore_signal(barrier, inc=1, device_id=to, device_id_type=MESH)
    pl.semaphore_wait(barrier, 3)
    give(0, ALL)

    def enter(slot, part, at, _):
        wide = rows_a[slot, at, :].astype(F32)
        a = (wide * norm_scale(wide, 1)).astype(BF)
        rows_a[slot, at, :] = a
        cols_a[slot, :, at] = a.T
        cols_d[slot, :, at] = rows_d[slot, at, :].T

    def first_pass(items):
        pass_on(0, items)
        give(1, items)

    def first_load():
        pass_across(0, ALL)
        gathered(0)
        load(0, 0)

    def entered(t, slot):
        return [(rows_a.at[slot], token_rows(a1, t)), (cols_a.at[slot], token_cols(a1t, t)), (cols_d.at[slot], token_cols(dyt, t))]

    passes(
        lambda t, s: [(token_rows(x, t), rows_a.at[s]), (token_rows(dy, t), rows_d.at[s])], entered, enter,
        [(1, lambda: first_pass(SOON)), (2, lambda: first_pass(LATER)), (3, first_load)],
    )

    steps = blocks * tiles

    def add_total(at, first, value):
        total[:, at] = value + jnp.where(first, 0.0, total[:, at])

    def f1_in(s, slot):
        return [(token_rows(a1, s % tiles), rows_a.at[slot])]

    def gu_out(s, slot):
        m, t = s // tiles, s % tiles
        return [(g_buf.at[slot], token_rows(g1.at[m], t)), (u_buf.at[slot], token_rows(u1.at[m], t))]

    def f2_dy(t, slot):
        return [(token_rows(dy, t), rows_d.at[slot]), (token_cols(dyt, t), cols_d.at[slot])]

    def f2_first(t, slot):
        return [*f2_dy(t, slot), (token_rows(x, t), rows_a.at[slot])]

    def f2_in(t, slot):
        return [*f2_dy(t, slot), (token_rows(a2, t), rows_a.at[slot]), (token_cols(a2t, t), cols_a.at[slot])]

    def f1_step(s, _):
        m, t, slot = s // tiles, s % tiles, s % 2
        gather_ticks(m, t)

        @pl.when(t == 0)
        def _():
            loaded(m % 2)

        @pl.when(s == 0)
        def _():
            wait(entered(tiles - 1, (tiles - 1) % 2), (tiles - 1) % 2, phase_sem)

        @pl.when(s + 1 < steps)
        def _():
            start(f1_in(s + 1, 1 - slot), 1 - slot)

        @pl.when(s + 1 == steps)
        def _():
            start(f2_first(0, 0), 0)

        @pl.when(s >= 2)
        def _():
            wait(gu_out(s - 2, slot), slot, gu_sem)

        wait(f1_in(s, slot), slot)
        w = wgu.at[m % 2]
        for c in range(TILE // CHUNK):
            at = pl.ds(c * CHUNK, CHUNK)
            a = rows_a[slot, at, :]
            g, u = nn(a, w[0]), nn(a, w[1])
            g_buf[slot, at, :] = g
            u_buf[slot, at, :] = u
            act[at, :] = (g * sigmoid(g) * u).astype(BF)
        start(gu_out(s, slot), slot, gu_sem)
        add_total(pl.ds(aligned(t * TILE, TILE), TILE), m == 0, nt(wdt[...], act[...]))

    start(f1_in(0, 0), 0)
    lax.fori_loop(0, steps, f1_step, None)
    for s in (steps - 2, steps - 1):
        wait(gu_out(s, s % 2), s % 2, gu_sem)

    def fold_states(c, size, t, first_block, w):
        at = pl.ds(c * size, size)
        add_total(pl.ds(aligned(t * TILE + c * size, size), size), first_block, nt(w[0], dgu[0, at, :]) + nt(w[1], dgu[1, at, :]))

    def fold(p, first_step, slot):
        for j in range(2):
            acc_w[p, j] = nn(cols_a[slot], dgu[j]) + jnp.where(first_step, 0.0, acc_w[p, j])
        acc_d[p] = nn(cols_d[slot], act[...]) + jnp.where(first_step, 0.0, acc_d[p])

    def h1_out(t, h):
        for i in range(n):
            rows = h1t.at[pl.ds(i * depth, depth), :]
            yield pltpu.make_async_copy((s2_w, r2_w)[h].at[i // 2, i % 2], half_cols(rows, t, h), h1_sem.at[h, i])

    def f2_out(t, slot):
        return [(rows_a.at[slot], token_rows(a2, t)), (cols_a.at[slot], token_cols(a2t, t))]

    def turn(slot, h, part, at, tok):
        state = (rows_a[slot, at, :].T.astype(F32) + total[:, tok].astype(BF).astype(F32)).astype(BF)
        for i in range(n):
            (s2_w, r2_w)[h][i // 2, i % 2, :, part] = state[i * depth : (i + 1) * depth, :]
        wide = state.astype(F32)
        a = (wide * norm_scale(wide, 0)).astype(BF)
        cols_a[slot, :, at] = a
        rows_a[slot, at, :] = a.T

    def b1_more(s, slot):
        b, t = s // tiles, s % tiles
        return [
            (token_cols(a1t, t), cols_a.at[slot]),
            (token_rows(g1.at[b], t), g_buf.at[slot]), (token_rows(u1.at[b], t), u_buf.at[slot]),
        ]

    def b1_first(s, slot):
        return [*b1_more(s, slot), (token_cols(dyt, s % tiles), cols_d.at[slot])]

    def h1_in(t, h):
        return pltpu.make_async_copy(half_cols(h1t, t, h), rows_a.at[h, pl.ds(0, width), pl.ds(0, part_tile)], tall_sem.at[h])

    def f2_step(s, _):
        r, t, slot = s // tiles, s % tiles, s % 2
        m = blocks + r
        gather_ticks(m, t)

        @pl.when((t == 1) & (r >= 1))
        def _():
            reduce_middle(r - 1, SOON)

        @pl.when((t == 2) & (r >= 1))
        def _():
            reduce_middle(r - 1, LATER)

        @pl.when(t == 0)
        def _():
            loaded(m % 2)

        @pl.when((s >= 1) & (s <= tiles))
        def _():
            wait(f2_out(s - 1, 1 - slot), 1 - slot, phase_sem)

        @pl.when(s + 1 < tiles)
        def _():
            start(f2_first(t + 1, 1 - slot), 1 - slot)

        @pl.when((s + 1 >= tiles) & (s + 1 < steps))
        def _():
            start(f2_in((s + 1) % tiles, 1 - slot), 1 - slot)

        @pl.when(s + 1 == steps)
        def _():
            h1_in(0, 0).start()
            start(b1_first(0, 0), 0)

        @pl.when(r == 0)
        def _():
            wait(f2_first(t, slot), slot)
            for h in range(2):
                @pl.when(t >= 1)
                def _():
                    for copy in h1_out(t - 1, h):
                        copy.wait()

                strips(t, h, functools.partial(turn, slot, h))
                for copy in h1_out(t, h):
                    copy.start()
            start(f2_out(t, slot), slot, phase_sem)

        @pl.when(r >= 1)
        def _():
            wait(f2_in(t, slot), slot)

        w = wgu.at[m % 2]

        def products(c):
            at = pl.ds(c * CHUNK, CHUNK)
            a = rows_a[slot, at, :]
            return nn(a, w[0]), nn(a, w[1]), nn(rows_d[slot, at, :], wdt[...])

        def keep(c, values):
            at = pl.ds(c * CHUNK, CHUNK)
            act[at, :], dgu[0, at, :], dgu[1, at, :] = gated_back(*values)

        before = products(0)
        for c in range(1, TILE // CHUNK):
            now = products(c)
            keep(c - 1, before)
            before = now
        keep(TILE // CHUNK - 1, before)
        for h in range(2):
            fold_states(h, part_tile, t, r == 0, w)
        fold(r % 2, t == 0, slot)

        @pl.when(t == tiles - 1)
        def _():
            @pl.when(r == 0)
            def _():
                for h in range(2):
                    for copy in h1_out(t, h):
                        copy.wait()

            @pl.when(r >= 1)
            def _():
                reduce_end(r - 1)

            reduce_start(r)

    lax.fori_loop(0, steps, f2_step, None)

    def b1_in(s, slot):
        t = s % tiles
        return [*b1_more(s, slot), (token_cols(dh1t, t), cols_d.at[slot]), (token_rows(dh1, t), rows_d.at[slot])]

    def b1_out(t, slot):
        return [(rows_d.at[slot], token_rows(dh1, t)), (cols_d.at[slot], token_cols(dh1t, t))]

    def back(state, grad, da, axis):
        through = norm_back(state, da.astype(F32), axis)
        return (grad.astype(F32) + through.astype(BF).astype(F32)).astype(BF)

    def turn_back(slot, h, part, at, tok):
        d = back(rows_a[h, pl.ds(0, width), part], cols_d[slot, :, at], total[:, tok].astype(BF), 0)
        cols_d[slot, :, at] = d
        rows_d[slot, at, :] = d.T

    def b1_body(slot, b, t, w, states, weights):
        def product(c):
            return nn(rows_d[slot, pl.ds(c * CHUNK, CHUNK), :], wdt[...])

        def keep(c, d):
            at = pl.ds(c * CHUNK, CHUNK)
            act[at, :], dgu[0, at, :], dgu[1, at, :] = gated_back(g_buf[slot, at, :], u_buf[slot, at, :], d)
            if states:
                fold_states(c, CHUNK, t, b == 0, w)

        before = product(0)
        for c in range(1, TILE // CHUNK):
            now = product(c)
            keep(c - 1, before)
            before = now
        keep(TILE // CHUNK - 1, before)
        if weights:
            fold((blocks + b) % 2, t == 0, slot)

    def end_in(t, slot):
        return [
            (token_rows(x, t), rows_a.at[slot]),
            (token_rows(g1.at[blocks - 1], t), g_buf.at[slot]), (token_rows(u1.at[blocks - 1], t), u_buf.at[slot]),
        ]

    def end_rows(t, slot):
        return pltpu.make_async_copy(token_rows(dh1, t), rows_d.at[slot], tall_sem.at[slot])

    def b1_step(final, s, _):
        b, t, slot = s // tiles, s % tiles, s % 2
        m, r = gathers + b, blocks + b

        @pl.when((t == 1) & (b + 1 < blocks))
        def _():
            load(b + 1, (m + 1) % 2)

        @pl.when(t == 1)
        def _():
            reduce_middle(r - 1, SOON)

        @pl.when(t == 2)
        def _():
            reduce_middle(r - 1, LATER)

        @pl.when(t == 0)
        def _():
            loaded(m % 2)

        if not final:
            @pl.when((s >= 1) & (s <= tiles))
            def _():
                wait(b1_out(s - 1, 1 - slot), 1 - slot, phase_sem)

            @pl.when(s + 1 < tiles)
            def _():
                start(b1_first(s + 1, 1 - slot), 1 - slot)

        @pl.when((s + 1 >= tiles) & (s + 1 < steps))
        def _():
            start(b1_in(s + 1, 1 - slot), 1 - slot)

        if final:
            @pl.when(s + 1 == steps)
            def _():
                start(end_in(0, 0), 0)
                end_rows(0, 0).start()

            wait(b1_in(s, slot), slot)
        else:
            @pl.when(b == 0)
            def _():
                wait(b1_first(s, slot), slot)
                for h in range(2):
                    h1_in(t, h).wait()
                    strips(t, h, functools.partial(turn_back, slot, h))

                    @pl.when(t + 1 < tiles)
                    def _():
                        h1_in(t + 1, h).start()

                start(b1_out(t, slot), slot, phase_sem)

            @pl.when(b >= 1)
            def _():
                wait(b1_in(s, slot), slot)

        b1_body(slot, b, t, wgu.at[m % 2], not final, True)

        @pl.when(t == tiles - 1)
        def _():
            reduce_end(r - 1)
            reduce_start(r)

    h1_in(0, 1).start()
    lax.fori_loop(0, steps - tiles, functools.partial(b1_step, False), None)
    lax.fori_loop(steps - tiles, steps, functools.partial(b1_step, True), None)

    last = layers * blocks - 1

    def leave(slot, part, at, tok):
        rows_d[slot, at, :] = back(rows_a[slot, at, :], rows_d[slot, at, :], total[:, tok].astype(BF).T, 1)

    def left_out(t, slot):
        return [(rows_d.at[slot], token_rows(dx, t))]

    def end_step(t, _):
        slot = t % 2

        @pl.when(t + 1 < tiles)
        def _():
            start(end_in(t + 1, 1 - slot), 1 - slot)

        wait(end_in(t, slot), slot)
        end_rows(t, slot).wait()
        b1_body(slot, blocks - 1, t, wgu.at[(gathers + blocks - 1) % 2], True, False)

        @pl.when(t >= 1)
        def _():
            wait(left_out(t - 1, 1 - slot), 1 - slot, phase_sem)

        @pl.when(t + 1 < tiles)
        def _():
            end_rows(t + 1, 1 - slot).start()

        for h in range(2):
            strips(t, h, functools.partial(leave, slot))
        start(left_out(t, slot), slot, phase_sem)

        @pl.when(t == 0)
        def _():
            reduce_middle(last, SOON)

        @pl.when(t == 1)
        def _():
            reduce_middle(last, LATER)

    lax.fori_loop(0, tiles, end_step, None)
    wait(left_out(tiles - 1, (tiles - 1) % 2), (tiles - 1) % 2, phase_sem)
    reduce_end(last)
    for copy in result_copies(last):
        copy.wait()
    for m in range(max(gathers - 4, 0), gathers):
        for k in range(5):
            sends_done(k, m, ALL)


def solution(mesh):
    n = mesh.shape["dp"]

    def local(x, dy, wg, wu, wd):
        tokens, width = x.shape[1:]
        layers, depth, ff = wg.shape
        span = n * LANES
        blocks = ff // span
        assert n == 4 and layers == 2 and mesh.shape["rep"] % 2 == 0
        assert ff % span == 0 and tokens % TILE == 0 and tokens // TILE == 4
        wide, tall = jax.ShapeDtypeStruct((tokens, width), BF), jax.ShapeDtypeStruct((width, tokens), BF)
        kept = jax.ShapeDtypeStruct((blocks, tokens, span), F32)
        grads = [jax.ShapeDtypeStruct(w.shape, w.dtype) for w in (wg, wu, wd)]
        hbm = [
            wide, tall, tall, tall, wide, tall, wide, tall, kept, kept,
            jax.ShapeDtypeStruct((layers * blocks, 2, width, span), BF), jax.ShapeDtypeStruct((layers * blocks, span, width), BF),
        ]
        outs = [wide, *grads, *hbm]
        dma = pltpu.SemaphoreType.DMA
        flops = 2 * tokens * width * ff * (9 * layers - 1)
        got = pl.pallas_call(
            functools.partial(kernel, n),
            out_shape=outs,
            in_specs=[pl.BlockSpec(memory_space=pl.ANY)] * 5,
            out_specs=[pl.BlockSpec(memory_space=pl.ANY)] * len(outs),
            scratch_shapes=[
                pltpu.VMEM((width, tokens), F32),
                pltpu.VMEM((2, 2, width, span), F32), pltpu.VMEM((2, width, span), F32),
                pltpu.VMEM((2, 2, width, span), BF), pltpu.VMEM((span, width), BF), pltpu.VMEM((width, span), BF),
                pltpu.VMEM((2, TILE, width), BF), pltpu.VMEM((2, TILE, width), BF),
                pltpu.VMEM((2, width, TILE), BF), pltpu.VMEM((2, width, TILE), BF),
                pltpu.VMEM((2, TILE, span), F32), pltpu.VMEM((2, TILE, span), F32),
                pltpu.VMEM((TILE, span), BF), pltpu.VMEM((2, TILE, span), BF),
                pltpu.VMEM((2, depth, span), BF), pltpu.VMEM((width, LANES), BF),
                pltpu.VMEM((2, 2, depth, span), BF), pltpu.VMEM((2, width, LANES), BF),
                pltpu.VMEM((2, 2, depth, span), BF), pltpu.VMEM((2, width, LANES), BF),
                pltpu.VMEM((2, depth, span), BF), pltpu.VMEM((LANES, width), BF),
                dma((5, 3, 4)), dma((5, 3, layers * blocks)), dma((2,)), dma((5, 2)), dma((2, 2)), dma((5, 2)), dma((2,)), dma((2, n)),
                dma((2, 2, 3)), dma((2, 2, 3)), dma((3, n)),
            ],
            compiler_params=pltpu.CompilerParams(collective_id=0, has_side_effects=True, vmem_limit_bytes=67043328),
            cost_estimate=pl.CostEstimate(flops=flops, bytes_accessed=0, transcendentals=0),
            name="stack",
        )(x[0], dy[0], wg, wu, wd)
        return (got[0][None], *got[1:4])

    tok, row = P(("rep", "dp"), None, None), P(None, "dp", None)
    return jax.shard_map(
        local, mesh=mesh, in_specs=(tok, tok, row, row, row), out_specs=(tok, *[P("rep", "dp", None)] * 3), check_vma=False
    )
```
